32 devices in a mesh: row: 4 (over y, x), col: 8 (over z, core).
Axes of the slice: x: 2, y: 2, z: 4, core: 2. Of those that a mesh axis runs over, the one named last changes fastest.
Arguments:
- features: bfloat16 [8192, 512], P(('row', 'col')), may hold values from -6 to 6
- tile_values: bfloat16 [4, 8, 128, 128, 128], P('row', 'col'), may hold values from -0.1875 to 0.1875
- tile_places: int32 [4, 8, 2, 128], P('row', 'col'), may hold values from 0 to 15, as said below
- tile_counts: int32 [4, 8], replicated, may hold values from 40 to 128, as said below
- weight_one: float32 [512, 512], replicated, may hold values from -0.25 to 0.25
- weight_two: float32 [512, 512], replicated, may hold values from -0.25 to 0.25
Outputs:
- embedded: float32 [8192, 512], P(('row', 'col'))
The draws below stay inside these ranges and needn't reach their ends.
Inputs may be any that keep to these rules, and one draw needn't show every extreme that they name: `tile_places`: in every block the first tile_counts slots name distinct tiles with tile rows below 16 and tile columns below 8, listed in order of tile row (never falling); later slots also name tiles in range. `tile_counts`: some block has exactly 128 tiles.
All inputs are finite; a program needn't handle non-finite values.
Results may differ from the reference program's by a relative error of at most 0.0029.
Values may be sent and summed in bfloat16 or wider, within the bound.
A program may use at most 64 MiB of HBM per device.

```python
import jax
import jax.numpy as jnp
from jax import lax

F = 512
TILE = 128
TR = 16
TC = 8
MAXT = 128
LOW = 40
PIECE = 256
ITEMS = 8192
N_ROW = 4
N_COL = 8


def block_counts(key):
    base_key = jax.random.fold_in(key, 11)
    first_key, second_key = jax.random.split(base_key)
    counts = jax.random.randint(first_key, (N_ROW * N_COL,), LOW, MAXT + 1)
    fullest = jax.random.randint(second_key, (), 0, N_ROW * N_COL)
    counts = jnp.where(jnp.arange(N_ROW * N_COL) == fullest, MAXT, counts)
    return counts.astype(jnp.int32)


def draw_tile_places(key, part):
    counts = block_counts(key)
    device_keys = jax.random.split(jax.random.fold_in(key, 23), N_ROW * N_COL)

    def draw_one(device_key, count):
        ordering = jax.random.permutation(device_key, TR * TC)[:MAXT]
        slots = jnp.arange(MAXT)
        keyed = jnp.where(slots < count, ordering, ordering + TR * TC)
        ranked = jnp.sort(keyed)
        chosen = jnp.where(ranked >= TR * TC, ranked - TR * TC, ranked)
        return jnp.stack([chosen // TC, chosen % TC]).astype(jnp.int32)
    return jax.vmap(draw_one)(device_keys, counts).reshape(N_ROW, N_COL, 2, MAXT)


def draw_tile_counts(key, part):
    return block_counts(key).reshape(N_ROW, N_COL)


def shard_levels(rng, dims, cuts, least, top_value):
    def one(axis_at, parts):
        heights = jax.random.uniform(jax.random.fold_in(jax.random.fold_in(rng, 6), axis_at), (parts,), jnp.float32, least / len(cuts), top_value / len(cuts))
        return jnp.repeat(jnp.exp(heights), dims[axis_at] // parts).reshape((-1,) + (1,) * (len(dims) - axis_at - 1))

    factor_of = one(*cuts[0])
    for cut in cuts[1:]:
        factor_of = factor_of * one(*cut)
    return factor_of


def scatter_about(rng, shape, width, reach, shards=(), held_as=jnp.bfloat16):
    result = jax.random.normal(rng, shape, jnp.float32) * width
    if len(shards) > 0:
        result = shard_levels(rng, shape, shards, -0.22, 0.18) * result
    return jnp.clip(result, min=-reach, max=reach).astype(held_as)


def setup_inputs(seed: int = 0) -> dict:
    splits = jax.random.split(jax.random.key(seed), 7)
    return {
        "features": scatter_about(splits[0], (ITEMS, F), 1.0, 6.0, ((0, 32),)),
        "tile_values": scatter_about(splits[1], (N_ROW, N_COL, MAXT, TILE, TILE), (MAXT * TILE // TR) ** -0.5, 0.1875, ((0, 4), (1, 8))),
        "tile_places": draw_tile_places(jax.random.fold_in(splits[6], 71), 0),
        "tile_counts": draw_tile_counts(jax.random.fold_in(splits[6], 71), 0),
        "weight_one": scatter_about(splits[4], (F, F), F ** -0.5, 0.25, (), jnp.float32),
        "weight_two": scatter_about(splits[5], (F, F), F ** -0.5, 0.25, (), jnp.float32),
    }


def aggregate(tile_values, tile_places, tile_counts, inputs):
    feature_blocks = inputs.reshape(N_ROW, N_COL, PIECE, F)
    all_values = tile_values.reshape(N_ROW * N_COL, MAXT, TILE, TILE)
    all_places = tile_places.reshape(N_ROW * N_COL, 2, MAXT)
    all_counts = tile_counts.reshape(N_ROW * N_COL)

    def one_block(totals, device_id):
        block_row = device_id // N_COL
        block_col = device_id % N_COL
        gathered = lax.dynamic_index_in_dim(feature_blocks, block_col, 1, keepdims=False)
        column_tiles = gathered.reshape(TC, TILE, F).astype(jnp.float32)
        blocks = all_values[device_id].astype(jnp.float32)
        places = all_places[device_id]
        active = (jnp.arange(MAXT, dtype=jnp.int32) < all_counts[device_id]).astype(jnp.float32)
        products = jnp.einsum("sij,sjf->sif", blocks, column_tiles[places[1]]) * active[:, None, None]
        partial_value = jnp.zeros((TR, TILE, F), jnp.float32).at[places[0]].add(products)
        return totals.at[block_row].add(partial_value), None

    start_totals = jnp.zeros((N_ROW, TR, TILE, F), jnp.float32)
    totals, _ = lax.scan(one_block, start_totals, jnp.arange(N_ROW * N_COL, dtype=jnp.int32))
    return totals.reshape(ITEMS, F)


def reference(features, tile_values, tile_places, tile_counts, weight_one, weight_two):
    first = aggregate(tile_values, tile_places, tile_counts, features)
    hidden = jnp.maximum(jnp.dot(first, weight_one, precision=lax.Precision.HIGHEST), 0.0).astype(jnp.bfloat16)
    second = aggregate(tile_values, tile_places, tile_counts, hidden)
    return jnp.maximum(jnp.dot(second, weight_two, precision=lax.Precision.HIGHEST), 0.0)
```

```python
import functools

import jax
import jax.numpy as jnp
from jax import lax
from jax.experimental import pallas as pl
from jax.experimental.pallas import tpu as pltpu
from jax.sharding import PartitionSpec as P

MESH = pl.DeviceIdType.MESH
PARTS = 2
LINK_TYPES = (jnp.float32, jnp.bfloat16)


def kernel(
    n_row, n_col,
    inverse_ref, features_ref, tiles_hbm, weight_one_hbm, weight_two_hbm,
    out_ref,
    tiles, dense, weights, hidden, inputs, own, total,
    pair_out, pair_in, up_out0, up_in0, down_out0, down_in0, up_out1, up_in1, down_out1, down_in1,
    load_sem, gather_send, gather_recv, pair_send, pair_recv, up_send, up_recv, down_send, down_recv,
):
    row, col = lax.axis_index("row"), lax.axis_index("col")
    n_chip = n_col // 2
    chip, core = col // 2, col % 2
    partner = chip * 2 + (1 - core)
    slots, tile = tiles_hbm.shape[0], tiles_hbm.shape[1]
    piece, width = features_ref.shape
    part = width // PARTS
    tile_rows, tile_cols = dense.shape[0] // tile, dense.shape[1] // tile

    tile_load = pltpu.make_async_copy(tiles_hbm, tiles.at[pl.ds(0, slots)], load_sem.at[0])
    tile_load.start()
    weight_loads = [
        pltpu.make_async_copy(weight_one_hbm, weights.at[0], load_sem.at[1]),
        pltpu.make_async_copy(weight_two_hbm, weights.at[1], load_sem.at[2]),
    ]
    for load in weight_loads:
        load.start()

    barrier = pltpu.get_barrier_semaphore()
    for step in range(1, n_row):
        pl.semaphore_signal(
            barrier, inc=1, device_id=(lax.rem(row + step, n_row), col), device_id_type=MESH
        )
    pl.semaphore_signal(barrier, inc=1, device_id=(row, partner), device_id_type=MESH)

    @pl.when(chip > 0)
    def _():
        pl.semaphore_signal(barrier, inc=1, device_id=(row, col - 2), device_id_type=MESH)

    @pl.when(chip < n_chip - 1)
    def _():
        pl.semaphore_signal(barrier, inc=1, device_id=(row, col + 2), device_id_type=MESH)

    peers = n_row + jnp.where(chip > 0, 1, 0) + jnp.where(chip < n_chip - 1, 1, 0)
    pl.semaphore_wait(barrier, peers)

    def gather_copy(layer, source, h, step):
        return pltpu.make_async_remote_copy(
            src_ref=source.at[:, pl.ds(h * part, part)],
            dst_ref=inputs.at[layer, h, pl.ds(pl.multiple_of(row * piece, piece), piece), :],
            send_sem=gather_send.at[layer, h, step - 1],
            recv_sem=gather_recv.at[layer, h, step - 1],
            device_id=(lax.rem(row + step, n_row), col),
            device_id_type=MESH,
        )

    def pair_copy(layer, h, d):
        return pltpu.make_async_remote_copy(
            src_ref=pair_out.at[layer, h, d],
            dst_ref=pair_in.at[layer, h, d],
            send_sem=pair_send.at[layer, h, d],
            recv_sem=pair_recv.at[layer, h, d],
            device_id=(row, partner),
            device_id_type=MESH,
        )

    ups = ((up_out0, up_in0), (up_out1, up_in1))
    downs = ((down_out0, down_in0), (down_out1, down_in1))

    def up_copy(layer, h, j):
        return pltpu.make_async_remote_copy(
            src_ref=ups[layer][0].at[h, j],
            dst_ref=ups[layer][1].at[h, j],
            send_sem=up_send.at[layer, h, j],
            recv_sem=up_recv.at[layer, h, j],
            device_id=(row, col + 2),
            device_id_type=MESH,
        )

    def down_copy(layer, h, j):
        return pltpu.make_async_remote_copy(
            src_ref=downs[layer][0].at[h, j],
            dst_ref=downs[layer][1].at[h, j],
            send_sem=down_send.at[layer, h, j],
            recv_sem=down_recv.at[layer, h, j],
            device_id=(row, col - 2),
            device_id_type=MESH,
        )

    def pair_sum(layer, h, d):
        pair_copy(layer, h, d).wait_recv()
        return own[h, d] + pair_in[layer, h, d]

    def send_up(layer, h, j, first):
        d = n_chip - 1 - j

        @pl.when(d > chip)
        def _():
            value = pair_sum(layer, h, d)
            if not first:
                up_copy(layer, h, j).wait_recv()
                value = value + ups[layer][1][h, j].astype(jnp.float32)
            ups[layer][0][h, j] = value.astype(LINK_TYPES[layer])
            up_copy(layer, h, j).start()

    def send_down(layer, h, j, first):
        d = j

        @pl.when(d < chip)
        def _():
            value = pair_sum(layer, h, d)
            if not first:
                down_copy(layer, h, j).wait_recv()
                value = value + downs[layer][1][h, j].astype(jnp.float32)
            downs[layer][0][h, j] = value.astype(LINK_TYPES[layer])
            down_copy(layer, h, j).start()

    def start_gather(layer, source):
        for h in range(PARTS):
            for step in range(1, n_row):
                gather_copy(layer, source, h, step).start()
        for h in range(PARTS):
            inputs[layer, h, pl.ds(pl.multiple_of(row * piece, piece), piece), :] = source[
                :, h * part : (h + 1) * part
            ]

    def chunk(layer, h, index):
        rows = pl.ds(pl.multiple_of(index * piece, piece), piece)
        return jnp.dot(dense[rows, :], inputs[layer, h], preferred_element_type=jnp.float32)

    def aggregate(layer, source):
        for h in range(PARTS):
            for step in range(1, n_row):
                gather_copy(layer, source, h, step).wait_recv()

            def one_chunk(i, carry):
                d = jnp.where(i % 2 == 0, n_chip - 1 - i // 2, i // 2)
                pair_out[layer, h, d] = chunk(layer, h, d * 2 + (1 - core))
                pair_copy(layer, h, d).start()
                own[h, d] = chunk(layer, h, d * 2 + core)
                return carry

            lax.fori_loop(0, n_chip, one_chunk, 0)

            @pl.when(chip == 0)
            def _():
                lax.fori_loop(0, n_chip - 1, lambda j, c: (send_up(layer, h, j, True), c)[1], 0)

            @pl.when(chip == n_chip - 1)
            def _():
                lax.fori_loop(0, n_chip - 1, lambda j, c: (send_down(layer, h, j, True), c)[1], 0)

        for h in range(PARTS):

            def forward(j, carry):
                @pl.when(chip > 0)
                def _():
                    send_up(layer, h, j, False)

                @pl.when(chip < n_chip - 1)
                def _():
                    send_down(layer, h, j, False)

                return carry

            lax.fori_loop(0, n_chip - 1, forward, 0)
        for h in range(PARTS):
            columns = slice(h * part, (h + 1) * part)
            total[:, columns] = pair_sum(layer, h, chip)

            @pl.when(chip > 0)
            def _():
                j = n_chip - 1 - chip
                up_copy(layer, h, j).wait_recv()
                total[:, columns] += ups[layer][1][h, j].astype(jnp.float32)

            @pl.when(chip < n_chip - 1)
            def _():
                down_copy(layer, h, chip).wait_recv()
                total[:, columns] += downs[layer][1][h, chip].astype(jnp.float32)

    def project(layer):
        product = jnp.dot(
            total[...], weights[layer], precision=lax.Precision.HIGHEST,
            preferred_element_type=jnp.float32,
        )
        return jnp.maximum(product, 0.0)

    start_gather(0, features_ref)
    tiles[slots] = jnp.zeros((tile, tile), tiles.dtype)
    tile_load.wait()

    def place_row(i, carry):
        rows = pl.ds(pl.multiple_of(i * tile, tile), tile)
        for t in range(tile_cols):
            slot = inverse_ref[i * tile_cols + t]
            dense[rows, t * tile : (t + 1) * tile] = tiles[slot]
        return carry

    lax.fori_loop(0, tile_rows, place_row, 0)
    for load in weight_loads:
        load.wait()

    aggregate(0, features_ref)
    hidden[...] = project(0).astype(hidden.dtype)
    start_gather(1, hidden)
    aggregate(1, hidden)
    out_ref[...] = project(1)

    for layer, source in enumerate((features_ref, hidden)):
        for h in range(PARTS):
            for step in range(1, n_row):
                gather_copy(layer, source, h, step).wait_send()

            def drain_pair(d, carry):
                pair_copy(layer, h, d).wait_send()
                return carry

            lax.fori_loop(0, n_chip, drain_pair, 0)

            def drain(j, carry):
                @pl.when(n_chip - 1 - j > chip)
                def _():
                    up_copy(layer, h, j).wait_send()

                @pl.when(j < chip)
                def _():
                    down_copy(layer, h, j).wait_send()

                return carry

            lax.fori_loop(0, n_chip - 1, drain, 0)


def shards(n_row, n_col, features, tile_values, tile_places, tile_counts, weight_one, weight_two):
    tiles = tile_values.reshape(tile_values.shape[2:])
    places = tile_places.reshape(tile_places.shape[2:])
    slots, tile = tiles.shape[0], tiles.shape[1]
    piece, width = features.shape
    part = width // PARTS
    rows, depth = piece * n_col, piece * n_row
    tile_rows, tile_cols = rows // tile, depth // tile
    n_chip = n_col // 2
    count = tile_counts[lax.axis_index("row"), lax.axis_index("col")]
    order = jnp.arange(slots, dtype=jnp.int32)
    position = jnp.where(order < count, places[0] * tile_cols + places[1], -1)
    spots = jnp.arange(tile_rows * tile_cols, dtype=jnp.int32)
    inverse = slots + jnp.sum(
        jnp.where(position[None, :] == spots[:, None], order[None, :] - slots, 0), axis=1
    )

    def flow(layer):
        return pltpu.VMEM((PARTS, n_chip - 1, piece, part), LINK_TYPES[layer])

    dma = pltpu.SemaphoreType.DMA
    any_space = pl.BlockSpec(memory_space=pl.ANY)
    vmem = pl.BlockSpec(memory_space=pltpu.VMEM)
    return pl.pallas_call(
        functools.partial(kernel, n_row, n_col),
        out_shape=jax.ShapeDtypeStruct((piece, width), jnp.float32),
        in_specs=[pl.BlockSpec(memory_space=pltpu.SMEM), vmem, any_space, any_space, any_space],
        out_specs=vmem,
        scratch_shapes=[
            pltpu.VMEM((slots + 1, tile, tile), jnp.bfloat16),
            pltpu.VMEM((rows, depth), jnp.bfloat16),
            pltpu.VMEM((2, width, width), jnp.float32),
            pltpu.VMEM((piece, width), jnp.bfloat16),
            pltpu.VMEM((2, PARTS, depth, part), jnp.bfloat16),
            pltpu.VMEM((PARTS, n_chip, piece, part), jnp.float32),
            pltpu.VMEM((piece, width), jnp.float32),
            pltpu.VMEM((2, PARTS, n_chip, piece, part), jnp.float32),
            pltpu.VMEM((2, PARTS, n_chip, piece, part), jnp.float32),
            flow(0), flow(0), flow(0), flow(0), flow(1), flow(1), flow(1), flow(1),
            dma((3,)),
            dma((2, PARTS, n_row - 1)), dma((2, PARTS, n_row - 1)),
            dma((2, PARTS, n_chip)), dma((2, PARTS, n_chip)),
            dma((2, PARTS, n_chip - 1)), dma((2, PARTS, n_chip - 1)),
            dma((2, PARTS, n_chip - 1)), dma((2, PARTS, n_chip - 1)),
        ],
        compiler_params=pltpu.CompilerParams(
            collective_id=0, has_side_effects=True, vmem_limit_bytes=60 * 1024 * 1024
        ),
    )(inverse, features, tiles, weight_one, weight_two)


def solution(mesh):
    placed = (
        P(("row", "col"), None),
        P("row", "col", None, None, None),
        P("row", "col", None, None),
        P(),
        P(),
        P(),
    )
    return jax.shard_map(
        functools.partial(shards, mesh.shape["row"], mesh.shape["col"]),
        mesh=mesh, in_specs=placed, out_specs=P(("row", "col"), None), check_vma=False,
    )
```

```python
import functools

import jax
import jax.numpy as jnp
from jax import lax
from jax.experimental import pallas as pl
from jax.experimental.pallas import tpu as pltpu
from jax.sharding import PartitionSpec as P

MESH = pl.DeviceIdType.MESH
PARTS = 4
LINK_TYPES = (jnp.int16, jnp.bfloat16)
TOP = 32766.0
SKEW = 2


def kernel(
    n_row, n_col,
    counts_ref, places_ref, features_ref, tiles_hbm, weight_one_hbm, weight_two_hbm,
    out_ref,
    tiles, dense, weights, hidden, inputs, own, total,
    pair_out, pair_in, up_out0, up_in0, down_out0, down_in0, up_out1, up_in1, down_out1, down_in1,
    scale_up_out, scale_up_in, scale_down_out, scale_down_in,
    load_sem, gather_send, gather_recv, pair_send, pair_recv, up_send, up_recv, down_send, down_recv,
    scale_send, scale_recv,
    inverse_rows, inverse_ref,
):
    row, col = lax.axis_index("row"), lax.axis_index("col")
    n_chip = n_col // 2
    chip, core = col // 2, col % 2
    partner = chip * 2 + (1 - core)
    slots, tile = tiles_hbm.shape[0], tiles_hbm.shape[1]
    piece, width = features_ref.shape
    part = width // PARTS
    tile_rows, tile_cols = dense.shape[0] // tile, dense.shape[1] // tile

    tile_load = pltpu.make_async_copy(tiles_hbm, tiles.at[pl.ds(0, slots)], load_sem.at[0])
    tile_load.start()
    weight_loads = [
        pltpu.make_async_copy(weight_one_hbm, weights.at[0], load_sem.at[1]),
        pltpu.make_async_copy(weight_two_hbm, weights.at[1], load_sem.at[2]),
    ]
    for load in weight_loads:
        load.start()

    barrier = pltpu.get_barrier_semaphore()
    for step in range(1, n_row):
        pl.semaphore_signal(
            barrier, inc=1, device_id=(lax.rem(row + step, n_row), col), device_id_type=MESH
        )
    pl.semaphore_signal(barrier, inc=1, device_id=(row, partner), device_id_type=MESH)

    @pl.when(chip > 0)
    def _():
        pl.semaphore_signal(barrier, inc=1, device_id=(row, col - 2), device_id_type=MESH)

    @pl.when(chip < n_chip - 1)
    def _():
        pl.semaphore_signal(barrier, inc=1, device_id=(row, col + 2), device_id_type=MESH)

    peers = n_row + jnp.where(chip > 0, 1, 0) + jnp.where(chip < n_chip - 1, 1, 0)
    pl.semaphore_wait(barrier, peers)

    def gather_copy(layer, source, h, step):
        return pltpu.make_async_remote_copy(
            src_ref=source.at[:, pl.ds(h * part, part)],
            dst_ref=inputs.at[layer, h, pl.ds(pl.multiple_of(row * piece, piece), piece), :],
            send_sem=gather_send.at[layer, h, step - 1],
            recv_sem=gather_recv.at[layer, h, step - 1],
            device_id=(lax.rem(row + step, n_row), col),
            device_id_type=MESH,
        )

    def pair_copy(layer, h, d):
        return pltpu.make_async_remote_copy(
            src_ref=pair_out.at[layer, h, d],
            dst_ref=pair_in.at[layer, h, d],
            send_sem=pair_send.at[layer, h, d],
            recv_sem=pair_recv.at[layer, h, d],
            device_id=(row, partner),
            device_id_type=MESH,
        )

    ups = ((up_out0, up_in0), (up_out1, up_in1))
    downs = ((down_out0, down_in0), (down_out1, down_in1))

    def up_copy(layer, h, j):
        return pltpu.make_async_remote_copy(
            src_ref=ups[layer][0].at[h, j],
            dst_ref=ups[layer][1].at[h, j],
            send_sem=up_send.at[layer, h, j],
            recv_sem=up_recv.at[layer, h, j],
            device_id=(row, col + 2),
            device_id_type=MESH,
        )

    def down_copy(layer, h, j):
        return pltpu.make_async_remote_copy(
            src_ref=downs[layer][0].at[h, j],
            dst_ref=downs[layer][1].at[h, j],
            send_sem=down_send.at[layer, h, j],
            recv_sem=down_recv.at[layer, h, j],
            device_id=(row, col - 2),
            device_id_type=MESH,
        )

    scales = ((scale_up_out, scale_up_in), (scale_down_out, scale_down_in))

    def scale_copy(way, h, j):
        return pltpu.make_async_remote_copy(
            src_ref=scales[way][0].at[h, j],
            dst_ref=scales[way][1].at[h, j],
            send_sem=scale_send.at[way, h, j],
            recv_sem=scale_recv.at[way, h, j],
            device_id=(row, col + 2 if way == 0 else col - 2),
            device_id_type=MESH,
        )

    def flow_copy(layer, way, h, j):
        return (up_copy, down_copy)[way](layer, h, j)

    def flow_send(layer, way, h, j, value):
        target = (ups, downs)[way][layer][0]
        if LINK_TYPES[layer] == jnp.int16:
            peak = jnp.maximum(jnp.max(jnp.abs(value), axis=0, keepdims=True), 1e-30)
            scales[way][0][h, j] = jnp.broadcast_to(peak * (1.0 / TOP), scales[way][0].shape[2:])
            scale_copy(way, h, j).start()
            target[h, j] = jnp.round(value * (TOP / peak)).astype(jnp.int32).astype(jnp.int16)
        else:
            target[h, j] = value.astype(target.dtype)
        flow_copy(layer, way, h, j).start()

    def flow_take(layer, way, h, j):
        source = (ups, downs)[way][layer][1]
        flow_copy(layer, way, h, j).wait_recv()
        if LINK_TYPES[layer] == jnp.int16:
            scale_copy(way, h, j).wait_recv()
            return source[h, j].astype(jnp.int32).astype(jnp.float32) * scales[way][1][h, j, 0:1, :]
        return source[h, j].astype(jnp.float32)

    def flow_drain(layer, way, h, j):
        flow_copy(layer, way, h, j).wait_send()
        if LINK_TYPES[layer] == jnp.int16:
            scale_copy(way, h, j).wait_send()

    def pair_sum(layer, h, d):
        pair_copy(layer, h, d).wait_recv()
        return own[h, d] + pair_in[layer, h, d]

    def send_up(layer, h, j, first):
        d = n_chip - 1 - j

        @pl.when(d > chip)
        def _():
            value = pair_sum(layer, h, d)
            if not first:
                value = value + flow_take(layer, 0, h, j)
            flow_send(layer, 0, h, j, value)

    def send_down(layer, h, j, first):
        d = j

        @pl.when(d < chip)
        def _():
            value = pair_sum(layer, h, d)
            if not first:
                value = value + flow_take(layer, 1, h, j)
            flow_send(layer, 1, h, j, value)

    def start_gather(layer, source):
        for h in range(PARTS):
            for step in range(1, n_row):
                gather_copy(layer, source, h, step).start()
        for h in range(PARTS):
            inputs[layer, h, pl.ds(pl.multiple_of(row * piece, piece), piece), :] = source[
                :, h * part : (h + 1) * part
            ]

    def chunk(layer, h, index):
        rows = pl.ds(pl.multiple_of(index * piece, piece), piece)
        return jnp.dot(dense[rows, :], inputs[layer, h], preferred_element_type=jnp.float32)

    def aggregate(layer, source):
        turns = n_chip - 1
        steps = PARTS * turns

        def forward(time, carry):
            for send, hops in ((send_up, chip), (send_down, turns - chip)):
                step = time - SKEW * hops

                @pl.when((step >= 0) & (step < steps) & (hops > 0))
                def _():
                    send(layer, step // turns, step % turns, False)

            return carry

        for h in range(PARTS):
            for step in range(1, n_row):
                gather_copy(layer, source, h, step).wait_recv()

            def one_chunk(i, carry):
                d = jnp.where(i % 2 == 0, n_chip - 1 - i // 2, i // 2)
                pair_out[layer, h, d] = chunk(layer, h, d * 2 + (1 - core))
                pair_copy(layer, h, d).start()
                own[h, d] = chunk(layer, h, d * 2 + core)
                return carry

            lax.fori_loop(0, n_chip, one_chunk, 0)

            @pl.when(chip == 0)
            def _():
                lax.fori_loop(0, n_chip - 1, lambda j, c: (send_up(layer, h, j, True), c)[1], 0)

            @pl.when(chip == n_chip - 1)
            def _():
                lax.fori_loop(0, n_chip - 1, lambda j, c: (send_down(layer, h, j, True), c)[1], 0)

            lax.fori_loop(h * turns, (h + 1) * turns, forward, 0)

        lax.fori_loop(steps, steps + SKEW * turns, forward, 0)
        for h in range(PARTS):
            columns = slice(h * part, (h + 1) * part)
            total[:, columns] = pair_sum(layer, h, chip)

            @pl.when(chip > 0)
            def _():
                total[:, columns] += flow_take(layer, 0, h, n_chip - 1 - chip)

            @pl.when(chip < n_chip - 1)
            def _():
                total[:, columns] += flow_take(layer, 1, h, chip)

    def project(layer):
        return jnp.dot(
            total[...], weights[layer], precision=lax.Precision.HIGHEST,
            preferred_element_type=jnp.float32,
        )

    start_gather(0, features_ref)
    tiles[slots] = jnp.zeros((tile, tile), tiles.dtype)
    spots = tile_rows * tile_cols
    count = counts_ref[row, col]
    order = lax.broadcasted_iota(jnp.int32, (spots, slots), 1)
    spot = lax.broadcasted_iota(jnp.int32, (spots, slots), 0)
    place = places_ref[0:1, :] * tile_cols + places_ref[1:2, :]
    listed = (place == spot) & (order < count)
    marks = jnp.where(listed, order - slots, 0)
    found = jnp.sum(marks.T, axis=0, keepdims=True) + slots
    inverse_rows[...] = jnp.broadcast_to(found, inverse_rows.shape)
    inverse_load = pltpu.make_async_copy(inverse_rows, inverse_ref, load_sem.at[3])
    inverse_load.start()
    inverse_load.wait()
    tile_load.wait()

    def place_row(i, carry):
        rows = pl.ds(pl.multiple_of(i * tile, tile), tile)
        for t in range(tile_cols):
            slot = jnp.clip(inverse_ref[0, i * tile_cols + t], 0, slots)
            dense[rows, t * tile : (t + 1) * tile] = tiles[slot]
        return carry

    lax.fori_loop(0, tile_rows, place_row, 0)
    for load in weight_loads:
        load.wait()

    aggregate(0, features_ref)
    hidden[...] = jnp.maximum(project(0), 0.0).astype(hidden.dtype)
    start_gather(1, hidden)
    aggregate(1, hidden)
    out_ref[...] = project(1)

    for layer, source in enumerate((features_ref, hidden)):
        for h in range(PARTS):
            for step in range(1, n_row):
                gather_copy(layer, source, h, step).wait_send()

            def drain_pair(d, carry):
                pair_copy(layer, h, d).wait_send()
                return carry

            lax.fori_loop(0, n_chip, drain_pair, 0)

            def drain(j, carry):
                @pl.when(n_chip - 1 - j > chip)
                def _():
                    flow_drain(layer, 0, h, j)

                @pl.when(j < chip)
                def _():
                    flow_drain(layer, 1, h, j)

                return carry

            lax.fori_loop(0, n_chip - 1, drain, 0)


def shards(n_row, n_col, features, tile_values, tile_places, tile_counts, weight_one, weight_two):
    tiles = tile_values.reshape(tile_values.shape[2:])
    places = tile_places.reshape(tile_places.shape[2:])
    slots, tile = tiles.shape[0], tiles.shape[1]
    piece, width = features.shape
    part = width // PARTS
    rows, depth = piece * n_col, piece * n_row
    tile_rows, tile_cols = rows // tile, depth // tile
    n_chip = n_col // 2
    spots = tile_rows * tile_cols

    def flow(layer):
        return pltpu.VMEM((PARTS, n_chip - 1, piece, part), LINK_TYPES[layer])

    scale = pltpu.VMEM((PARTS, n_chip - 1, 8, part), jnp.float32)
    dma = pltpu.SemaphoreType.DMA
    any_space = pl.BlockSpec(memory_space=pl.ANY)
    vmem = pl.BlockSpec(memory_space=pltpu.VMEM)
    second = pl.pallas_call(
        functools.partial(kernel, n_row, n_col),
        out_shape=jax.ShapeDtypeStruct((piece, width), jnp.float32),
        in_specs=[pl.BlockSpec(memory_space=pltpu.SMEM), vmem, vmem, any_space, any_space, any_space],
        out_specs=vmem,
        scratch_shapes=[
            pltpu.VMEM((slots + 1, tile, tile), jnp.bfloat16),
            pltpu.VMEM((rows, depth), jnp.bfloat16),
            pltpu.VMEM((2, width, width), jnp.float32),
            pltpu.VMEM((piece, width), jnp.bfloat16),
            pltpu.VMEM((2, PARTS, depth, part), jnp.bfloat16),
            pltpu.VMEM((PARTS, n_chip, piece, part), jnp.float32),
            pltpu.VMEM((piece, width), jnp.float32),
            pltpu.VMEM((2, PARTS, n_chip, piece, part), jnp.float32),
            pltpu.VMEM((2, PARTS, n_chip, piece, part), jnp.float32),
            flow(0), flow(0), flow(0), flow(0), flow(1), flow(1), flow(1), flow(1),
            scale, scale, scale, scale,
            dma((4,)),
            dma((2, PARTS, n_row - 1)), dma((2, PARTS, n_row - 1)),
            dma((2, PARTS, n_chip)), dma((2, PARTS, n_chip)),
            dma((2, PARTS, n_chip - 1)), dma((2, PARTS, n_chip - 1)),
            dma((2, PARTS, n_chip - 1)), dma((2, PARTS, n_chip - 1)),
            dma((2, PARTS, n_chip - 1)), dma((2, PARTS, n_chip - 1)),
            pltpu.VMEM((8, spots), jnp.int32), pltpu.SMEM((8, spots), jnp.int32),
        ],
        compiler_params=pltpu.CompilerParams(
            collective_id=0, has_side_effects=True, vmem_limit_bytes=60 * 1024 * 1024
        ),
    )(tile_counts, places, features, tiles, weight_one, weight_two)
    return jnp.maximum(second, 0.0)


def solution(mesh):
    placed = (
        P(("row", "col"), None),
        P("row", "col", None, None, None),
        P("row", "col", None, None),
        P(),
        P(),
        P(),
    )
    return jax.shard_map(
        functools.partial(shards, mesh.shape["row"], mesh.shape["col"]),
        mesh=mesh, in_specs=placed, out_specs=P(("row", "col"), None), check_vma=False,
    )
```
